32 devices in a mesh: sy: 4 (over y, x), sx: 4 (over z), wl: 2 (over core).
Axes of the slice: x: 2, y: 2, z: 4, core: 2. Of those that a mesh axis runs over, the one named last changes fastest.
Arguments:
- interface_map: bfloat16 [8, 4, 1536, 2, 1536], P(('wl', 'sy'), 'sx'), parts along dimension 0, may hold values from -0.0625 to 0.0625
- source_trace: float32 [8, 4, 2, 64, 4, 384], P(('wl', 'sy'), 'sx'), parts along dimension 0, may hold values from -6 to 6
- restriction: float32 [8, 4, 2, 32, 4, 384], P(('wl', 'sy'), 'sx'), parts along dimension 0, may hold values from -0.02734375 to 0.02734375
- prolongation: float32 [8, 4, 2, 32, 4, 384], P(('wl', 'sy'), 'sx'), parts along dimension 0, may hold values from -0.109375 to 0.109375
- coarse_inverse: float32 [4, 32, 32], P('wl'), parts along dimension 0, may hold values from -0.75 to 0.75
Outputs:
- traces: float32 [8, 4, 2, 64, 4, 384], P(('wl', 'sy'), 'sx'), parts along dimension 0
- coarse_coef: float32 [4, 64, 32], P('wl'), parts along dimension 0
The draws below stay inside these ranges and needn't reach their ends.
There are 2 independent parts, one for each index of `wl`. The reference program is written for one: setup_inputs(seed, part) draws one part's arguments, and reference() takes and returns one part's arrays. A program takes and returns all parts, laid end to end along the dimension named above; each array names one. Nothing has to cross between parts.
All inputs are finite; a program needn't handle non-finite values.
Results may differ from the reference program's by a relative error of at most 0.0025.
Values sent between devices are 32-bit elements; how exact they have to be, the bound alone decides.
A program may use at most 128 MiB of HBM per device.

```python
import jax
import jax.numpy as jnp
from jax import lax

M = 384
NC = 32
S = 64
ITERS = 6
SUBY = 4
SUBX = 4


def steps_of(stream_key, extent, cuts, low, top_value):
    loudness, own = 1.0, jax.random.fold_in(stream_key, 6)
    for position, parts in cuts:
        draws = jnp.exp(jax.random.uniform(jax.random.fold_in(own, position), (parts,), jnp.float32, low / len(cuts), top_value / len(cuts)))
        loudness = loudness * jnp.repeat(draws, extent[position] // parts).reshape([-1 if axis == position else 1 for axis in range(len(extent))])
    return loudness


def centred(key, extent, width, most, cuts=(), dtype=jnp.bfloat16):
    drawn = jax.random.normal(key, extent, jnp.float32) * width
    if len(cuts) > 0:
        drawn = steps_of(key, extent, cuts, -0.22, 0.18) * drawn
    return jnp.clip(drawn, min=-most, max=most).astype(dtype)


def setup_inputs(seed: int = 0, part: int = 0) -> dict:
    key_list = jax.random.split(jax.random.key(seed), 6)
    own_keys = jax.random.split(jax.random.fold_in(key_list[5], part), 6)
    return {
        "interface_map": centred(own_keys[0], (SUBY, SUBX, 4 * M, 2, 4 * M), (24 * M) ** -0.5, 0.0625, ((0, 4), (1, 4))),
        "source_trace": centred(own_keys[1], (SUBY, SUBX, 2, S, 4, M), 1.0, 6.0, ((0, 4), (1, 4)), jnp.float32),
        "restriction": centred(own_keys[2], (SUBY, SUBX, 2, NC, 4, M), (8 * M * SUBY * SUBX) ** -0.5, 0.02734375, ((0, 4), (1, 4)), jnp.float32),
        "prolongation": centred(own_keys[3], (SUBY, SUBX, 2, NC, 4, M), (96 * NC) ** -0.5, 0.109375, ((0, 4), (1, 4)), jnp.float32),
        "coarse_inverse": centred(own_keys[4], (2, NC, NC), (2 * NC) ** -0.5, 0.75, (), jnp.float32),
    }


PRECISE = lax.Precision.HIGHEST


def shifted(values, along, offset):
    length_axis = values.shape[along]
    blank_edge = jnp.zeros_like(lax.slice_in_dim(values, 0, 1, axis=along))
    if offset == 1:
        return jnp.concatenate([blank_edge, lax.slice_in_dim(values, 0, length_axis - 1, axis=along)], axis=along)
    return jnp.concatenate([lax.slice_in_dim(values, 1, length_axis, axis=along), blank_edge], axis=along)


def complex_pair(left_real, left_imag, right_real, right_imag, pattern):
    real_part = jnp.einsum(pattern, left_real, right_real, precision=PRECISE) - jnp.einsum(pattern, left_imag, right_imag, precision=PRECISE)
    imag_part = jnp.einsum(pattern, left_real, right_imag, precision=PRECISE) + jnp.einsum(pattern, left_imag, right_real, precision=PRECISE)
    return jnp.stack([real_part, imag_part])


def corner_values(outgoing):
    corner_northwest = outgoing[..., 0, 0] + outgoing[..., 2, 0]
    corner_northeast = outgoing[..., 0, -1] + outgoing[..., 3, 0]
    corner_southwest = outgoing[..., 1, 0] + outgoing[..., 2, -1]
    corner_southeast = outgoing[..., 1, -1] + outgoing[..., 3, -1]
    return corner_northwest, corner_northeast, corner_southwest, corner_southeast


def assemble(from_north, from_south, from_west, from_east, into_northwest, into_northeast, into_southwest, into_southeast):
    north_side = from_north.at[..., 0].add(0.5 * into_northwest).at[..., -1].add(0.5 * into_northeast)
    south_side = from_south.at[..., 0].add(0.5 * into_southwest).at[..., -1].add(0.5 * into_southeast)
    west_side = from_west.at[..., 0].add(0.5 * into_northwest).at[..., -1].add(0.5 * into_southwest)
    east_side = from_east.at[..., 0].add(0.5 * into_northeast).at[..., -1].add(0.5 * into_southeast)
    return jnp.stack([north_side, south_side, west_side, east_side], axis=-2)


def reference(interface_map, source_trace, restriction, prolongation, coarse_inverse):
    grid_rows, grid_cols = source_trace.shape[0], source_trace.shape[1]
    src_count, side_len = source_trace.shape[3], source_trace.shape[5]
    coarse_width = restriction.shape[3]
    flat_map = interface_map.reshape(grid_rows * grid_cols, 4 * side_len, 8 * side_len)
    rest_flat = restriction.reshape(grid_rows, grid_cols, 2, coarse_width, 4 * side_len)
    lift_flat = prolongation.reshape(grid_rows, grid_cols, 2, coarse_width, 4 * side_len)
    traces = jnp.zeros(source_trace.shape, jnp.float32)
    coef_now = jnp.zeros((2, src_count, coarse_width), jnp.float32)
    for sweep_index in range(ITERS):
        flat_traces = traces.reshape(grid_rows, grid_cols, 2, src_count, 4 * side_len)
        coarse_total = complex_pair(flat_traces[:, :, 0], flat_traces[:, :, 1], rest_flat[:, :, 0], rest_flat[:, :, 1], "yxsk,yxnk->sn")
        coef_now = complex_pair(coarse_total[0], coarse_total[1], coarse_inverse[0], coarse_inverse[1], "sn,nq->sq")
        spread = complex_pair(coef_now[0], coef_now[1], lift_flat[:, :, 0], lift_flat[:, :, 1], "sn,yxnk->yxsk")
        corrected = flat_traces + jnp.moveaxis(spread, 0, 2)
        row_block = corrected.astype(jnp.bfloat16).reshape(grid_rows * grid_cols, 2 * src_count, 4 * side_len)
        product = lax.map(lambda operands: jnp.dot(operands[0], operands[1], preferred_element_type=jnp.float32), (row_block, flat_map))
        product = product.reshape(grid_rows, grid_cols, 2, src_count, 2, 4 * side_len)
        real_part = product[:, :, 0, :, 0] - product[:, :, 1, :, 1]
        imag_part = product[:, :, 0, :, 1] + product[:, :, 1, :, 0]
        outgoing = jnp.stack([real_part, imag_part], axis=2).reshape(source_trace.shape) + source_trace
        from_north = shifted(outgoing[:, :, :, :, 1], 0, 1)
        from_south = shifted(outgoing[:, :, :, :, 0], 0, -1)
        from_west = shifted(outgoing[:, :, :, :, 3], 1, 1)
        from_east = shifted(outgoing[:, :, :, :, 2], 1, -1)
        corner_northwest, corner_northeast, corner_southwest, corner_southeast = corner_values(outgoing)
        into_northwest = shifted(shifted(corner_southeast, 0, 1), 1, 1)
        into_northeast = shifted(shifted(corner_southwest, 0, 1), 1, -1)
        into_southwest = shifted(shifted(corner_northeast, 0, -1), 1, 1)
        into_southeast = shifted(shifted(corner_northwest, 0, -1), 1, -1)
        traces = assemble(from_north, from_south, from_west, from_east, into_northwest, into_northeast, into_southwest, into_southeast)
    return traces, coef_now
```

```python
import functools

import jax
import jax.numpy as jnp
from jax import lax
from jax.experimental import pallas as pl
from jax.experimental.pallas import tpu as pltpu
from jax.sharding import PartitionSpec as P

ITERS = 6
LANES = 128
F32, BF16 = jnp.float32, jnp.bfloat16
MESH = pl.DeviceIdType.MESH
PRECISE = lax.Precision.HIGHEST
NT = (((1,), (1,)), ((), ()))


def dot(a, b):
    return jnp.dot(a, b, preferred_element_type=F32)


def dot_nt(a, b):
    return lax.dot_general(a, b, NT, preferred_element_type=F32)


def split(x):
    hi = x.astype(BF16)
    return hi, (x - hi.astype(F32)).astype(BF16)


def sweep_kernel(
    ny, nx, iters,
    map_ref, src_ref, rest_ref, lift_ref, inv_ref,
    traces_ref, coef_ref,
    out, recv, wrecv, cbuf, crecv, wcbuf, wcrecv, lhs, ext_lhs, ext_rhs,
    wts, part, xs, rowsum, ys,
    side_send, side_recv, diag_send, diag_recv,
    wside_send, wside_recv, wdiag_send, wdiag_recv,
    x_send, x_recv, y_send, y_recv,
):
    rows, k = src_ref.shape
    side = k // 4
    nsrc = rows // 2
    nw_rows = rest_ref.shape[0]
    nc = nw_rows // 2
    half = nsrc // 2
    y, x = lax.axis_index("sy"), lax.axis_index("sx")
    up, dn, lf, rt = y > 0, y < ny - 1, x > 0, x < nx - 1
    sides = ((up, -1, 0), (dn, 1, 0), (lf, 0, -1), (rt, 0, 1))
    diags = (
        (up & lf, -1, -1),
        (up & rt, -1, 1),
        (dn & lf, 1, -1),
        (dn & rt, 1, 1),
    )

    def lanes(s):
        return pl.ds(s * side, side)

    def copies(src, dst, corner_src, corner_dst, ssem, rsem, dsem, drsem):
        flat, diag, flat_in, diag_in = [], [], [], []
        for d, (cond, dy, dx) in enumerate(sides):
            o = d ^ 1
            dev = {"sy": y + dy, "sx": x + dx}
            flat.append((cond, pltpu.make_async_remote_copy(
                src.at[:, lanes(d)], dst.at[:, lanes(o)], ssem.at[d], rsem.at[o],
                device_id=dev, device_id_type=MESH)))
            flat_in.append((cond, pltpu.make_async_remote_copy(
                src.at[:, lanes(d)], dst.at[:, lanes(d)], ssem.at[d], rsem.at[d],
                device_id=dev, device_id_type=MESH)))
        for d, (cond, dy, dx) in enumerate(diags):
            o = 3 - d
            dev = {"sy": y + dy, "sx": x + dx}
            diag.append((cond, pltpu.make_async_remote_copy(
                corner_src, corner_dst.at[o], dsem.at[d], drsem.at[o],
                device_id=dev, device_id_type=MESH)))
            diag_in.append((cond, pltpu.make_async_remote_copy(
                corner_src, corner_dst.at[d], dsem.at[d], drsem.at[d],
                device_id=dev, device_id_type=MESH)))
        return flat, diag, flat_in, diag_in

    def each(items, what):
        for cond, c in items:
            pl.when(cond)(getattr(c, what))

    def pack_corners(ref, dst, scale):
        def column(s, last):
            if last:
                return ref[:, (s + 1) * side - LANES:(s + 1) * side][:, LANES - 1:]
            return ref[:, s * side:s * side + LANES][:, 0:1]

        n = ref.shape[0]
        lane = lax.broadcasted_iota(jnp.int32, (n, LANES), 1)
        block = jnp.zeros((n, LANES), F32)
        for j, (a, b) in enumerate((
            ((0, 0), (2, 0)), ((0, 1), (3, 0)), ((1, 0), (2, 1)), ((1, 1), (3, 1)),
        )):
            block = jnp.where(lane == j, column(*a) + column(*b), block)
        if scale != 1.0:
            block = block * scale
        if n < LANES:
            block = jnp.concatenate([block, jnp.zeros((LANES - n, LANES), F32)], axis=0)
        dst[...] = block.T[:8]

    def assemble(get, get_corner, n, scale, write):
        row = lax.broadcasted_iota(jnp.int32, (LANES, LANES), 0)
        block = jnp.zeros((LANES, LANES), F32)
        for j in range(4):
            block = jnp.where(row == j, get_corner(j)[3 - j:4 - j], block)
        cols = block.T[:n] * scale
        lane = lax.broadcasted_iota(jnp.int32, (n, LANES), 1)
        ends = ((0, 1), (2, 3), (0, 2), (1, 3))
        for s in range(4):
            for t in range(side // LANES):
                at = s * side + t * LANES
                v = get(at)
                if t == 0:
                    j = ends[s][0]
                    v = v + jnp.where(lane == 0, cols[:, j:j + 1], 0.0)
                if t == side // LANES - 1:
                    j = ends[s][1]
                    v = v + jnp.where(lane == LANES - 1, cols[:, j:j + 1], 0.0)
                write(at, v)

    for d, (cond, _, _) in enumerate(sides):
        @pl.when(jnp.logical_not(cond))
        def _(d=d):
            for slot in range(2):
                recv[slot, :, lanes(d)] = jnp.zeros((rows, side), F32)
            wrecv[:, lanes(d)] = jnp.zeros((nw_rows, side), F32)
    for d, (cond, _, _) in enumerate(diags):
        @pl.when(jnp.logical_not(cond))
        def _(d=d):
            for slot in range(2):
                crecv[slot, d] = jnp.zeros((8, LANES), F32)
            wcrecv[d] = jnp.zeros((8, LANES), F32)

    w_flat, w_diag, w_flat_in, w_diag_in = copies(
        rest_ref, wrecv, wcbuf, wcrecv, wside_send, wside_recv, wdiag_send, wdiag_recv)
    pack_corners(rest_ref, wcbuf, 0.5)
    each(w_diag, "start")
    each(w_flat, "start")

    def exchange(slot, src):
        return copies(
            src, recv.at[slot], cbuf.at[slot], crecv.at[slot],
            side_send.at[slot], side_recv.at[slot], diag_send.at[slot], diag_recv.at[slot])

    def x_copies(slot):
        res = []
        for d in range(1, nx):
            peer = lax.rem(x + d, nx)
            res.append((
                pltpu.make_async_remote_copy(
                    part.at[slot], xs.at[slot, x], x_send.at[slot, d], x_recv.at[slot, d],
                    device_id={"sy": y, "sx": peer}, device_id_type=MESH),
                pltpu.make_async_remote_copy(
                    part.at[slot], xs.at[slot, lax.rem(x + nx - d, nx)],
                    x_send.at[slot, d], x_recv.at[slot, d],
                    device_id={"sy": y, "sx": peer}, device_id_type=MESH)))
        return res

    def y_copies(slot):
        res = []
        for d in range(1, ny):
            peer = lax.rem(y + d, ny)
            res.append((
                pltpu.make_async_remote_copy(
                    rowsum.at[slot], ys.at[slot, y], y_send.at[slot, d], y_recv.at[slot, d],
                    device_id={"sy": peer, "sx": x}, device_id_type=MESH),
                pltpu.make_async_remote_copy(
                    rowsum.at[slot], ys.at[slot, lax.rem(y + ny - d, ny)],
                    y_send.at[slot, d], y_recv.at[slot, d],
                    device_id={"sy": peer, "sx": x}, device_id_type=MESH)))
        return res

    def restrict_start(slot, src):
        re_hi, re_lo = split(src[:nsrc])
        im_hi, im_lo = split(src[nsrc:])
        a_hi, a_lo, b_hi, b_lo = (wts[i] for i in range(4))
        t = dot_nt(re_hi, a_hi) + dot_nt(im_hi, b_hi)
        t = t + (dot_nt(re_lo, a_hi) + dot_nt(im_lo, b_hi))
        t = t + (dot_nt(re_hi, a_lo) + dot_nt(im_hi, b_lo))
        lane = lax.broadcasted_iota(jnp.int32, (half, LANES), 1)
        t = jnp.where(lane < 2 * nc, t[:half], t[half:])
        part[slot] = t
        xs[slot, x] = t
        for c, _ in x_copies(slot):
            c.start()

    def restrict_turn(slot):
        for _, c in x_copies(slot):
            c.wait_recv()
        t = xs[slot, 0]
        for i in range(1, nx):
            t = t + xs[slot, i]
        rowsum[slot] = t
        ys[slot, y] = t
        for c, _ in y_copies(slot):
            c.start()

    def coarse(slot):
        for _, c in y_copies(slot):
            c.wait_recv()
        t = ys[slot, 0]
        for i in range(1, ny):
            t = t + ys[slot, i]
        lane = lax.broadcasted_iota(jnp.int32, (half, LANES), 1)
        low = lane < 2 * nc
        t = jnp.concatenate([jnp.where(low, t, 0.0), jnp.where(low, 0.0, t)], axis=0)
        c_re = jnp.dot(t, inv_ref[0], preferred_element_type=F32, precision=PRECISE)
        c_im = jnp.dot(t, inv_ref[1], preferred_element_type=F32, precision=PRECISE)
        c = jnp.concatenate([c_re, c_im], axis=0)
        coef_ref[...] = c
        hi, lo = split(c)
        lane = lax.broadcasted_iota(jnp.int32, (rows, LANES), 1)
        mid = (lane >= nc) & (lane < 2 * nc)
        ext_lhs[...] = jnp.where(mid, lo.astype(F32), hi.astype(F32)).astype(BF16)

    def restrict_end(slot):
        for c, _ in x_copies(slot):
            c.wait_send()
        for c, _ in y_copies(slot):
            c.wait_send()

    flat, diag, flat_in, diag_in = exchange(0, src_ref)
    pack_corners(src_ref, cbuf.at[0], 1.0)
    each(diag, "start")
    each(flat, "start")

    lift_hi, lift_lo = split(lift_ref[...])
    lhs[...] = jnp.concatenate([lift_hi, lift_lo], axis=0)
    for s in range(4):
        p = dot(lhs[...], map_ref[:, s * side:(s + 1) * side])
        q = dot(lhs[...], map_ref[:, k + s * side:k + (s + 1) * side])
        p = p[:nw_rows] + p[nw_rows:]
        q = q[:nw_rows] + q[nw_rows:]
        for at, v in ((s * side, p[:nc] - q[nc:]), (k + s * side, q[:nc] + p[nc:])):
            hi, lo = split(v)
            ext_rhs[:, at:at + side] = jnp.concatenate(
                [hi, hi, lo, jnp.zeros((LANES - 3 * nc, side), BF16)], axis=0)

    each(w_flat_in, "wait_recv")
    each(w_diag_in, "wait_recv")

    def write_weights(at, v):
        wr, wi = v[:nc], v[nc:]
        for i, rowset in ((0, [wr, wi, wr, wi]), (2, [-wi, wr, -wi, wr])):
            hi, lo = split(jnp.concatenate(rowset, axis=0))
            wts[i, :, at:at + LANES] = hi
            wts[i + 1, :, at:at + LANES] = lo

    assemble(lambda at: wrecv[:, at:at + LANES], lambda j: wcrecv[j], nw_rows, 1.0, write_weights)
    restrict_start(0, src_ref)
    restrict_turn(0)
    each(w_flat, "wait_send")
    each(w_diag, "wait_send")

    def store_lhs(at, v):
        lhs[:, at:at + LANES] = v.astype(BF16)

    def step(it, carry):
        old = lax.rem(it + 1, 2)
        new = lax.rem(it, 2)
        flat, diag, flat_in, diag_in = exchange(old, out)
        each(diag_in, "wait_recv")
        each(flat_in, "wait_recv")
        assemble(lambda at: recv[old, :, at:at + LANES], lambda j: crecv[old, j], rows, 0.5, store_lhs)
        each(flat, "wait_send")
        each(diag, "wait_send")
        for s in range(4):
            at = s * side
            p = dot(lhs[...], map_ref[:, at:at + side])
            q = dot(lhs[...], map_ref[:, k + at:k + at + side])
            out[:nsrc, at:at + side] = p[:nsrc] - q[nsrc:] + src_ref[:nsrc, at:at + side]
            out[nsrc:, at:at + side] = q[:nsrc] + p[nsrc:] + src_ref[nsrc:, at:at + side]
        coarse(old)
        restrict_end(old)
        for s in range(4):
            at = s * side
            p = dot(ext_lhs[...], ext_rhs[:, at:at + side])
            q = dot(ext_lhs[...], ext_rhs[:, k + at:k + at + side])
            out[:nsrc, at:at + side] += p[:nsrc] - q[nsrc:]
            out[nsrc:, at:at + side] += q[:nsrc] + p[nsrc:]
        flat, diag, _, _ = exchange(new, out)
        pack_corners(out, cbuf.at[new], 1.0)
        each(diag, "start")

        @pl.when(it < iters - 1)
        def _():
            restrict_start(new, out)

        each(flat, "start")

        @pl.when(it < iters - 1)
        def _():
            restrict_turn(new)

        return carry

    lax.fori_loop(1, iters, step, 0)

    last = (iters - 1) % 2
    flat, diag, flat_in, diag_in = exchange(last, out)
    each(diag_in, "wait_recv")
    each(flat_in, "wait_recv")

    def store_out(at, v):
        traces_ref[:, at:at + LANES] = v

    assemble(lambda at: recv[last, :, at:at + LANES], lambda j: crecv[last, j], rows, 0.5, store_out)
    each(flat, "wait_send")
    each(diag, "wait_send")


def per_device(ny, nx, interface_map, source_trace, restriction, prolongation, coarse_inverse):
    _, _, _, nsrc, _, side = source_trace.shape
    nc = restriction.shape[3]
    k, rows = 4 * side, 2 * nsrc
    table = interface_map.reshape(k, 2 * k)
    src = source_trace.reshape(rows, k)
    rest = restriction.reshape(2 * nc, k)
    lift = prolongation.reshape(2 * nc, k)
    cr, ci = coarse_inverse[0], coarse_inverse[1]

    def spread(top, bottom):
        column = jnp.concatenate([top, bottom, top, bottom], axis=0)
        blank = jnp.zeros((4 * nc, LANES - 3 * nc), F32)
        return jnp.concatenate([column, column, column, blank], axis=1)

    inv = jnp.stack([spread(cr, -ci), spread(ci, cr)])
    half = nsrc // 2
    dma = pltpu.SemaphoreType.DMA
    vmem = pl.BlockSpec(memory_space=pltpu.VMEM)
    traces, coef = pl.pallas_call(
        functools.partial(sweep_kernel, ny, nx, ITERS),
        out_shape=(
            jax.ShapeDtypeStruct((rows, k), F32),
            jax.ShapeDtypeStruct((rows, LANES), F32),
        ),
        in_specs=[vmem] * 5,
        out_specs=(vmem, vmem),
        scratch_shapes=[
            pltpu.VMEM((rows, k), F32),
            pltpu.VMEM((2, rows, k), F32),
            pltpu.VMEM((2 * nc, k), F32),
            pltpu.VMEM((2, 8, LANES), F32),
            pltpu.VMEM((2, 4, 8, LANES), F32),
            pltpu.VMEM((8, LANES), F32),
            pltpu.VMEM((4, 8, LANES), F32),
            pltpu.VMEM((rows, k), BF16),
            pltpu.VMEM((rows, LANES), BF16),
            pltpu.VMEM((LANES, 2 * k), BF16),
            pltpu.VMEM((4, 4 * nc, k), BF16),
            pltpu.VMEM((2, half, LANES), F32),
            pltpu.VMEM((2, nx, half, LANES), F32),
            pltpu.VMEM((2, half, LANES), F32),
            pltpu.VMEM((2, ny, half, LANES), F32),
            dma((2, 4)), dma((2, 4)), dma((2, 4)), dma((2, 4)),
            dma((4,)), dma((4,)), dma((4,)), dma((4,)),
            dma((2, nx)), dma((2, nx)), dma((2, ny)), dma((2, ny)),
        ],
        compiler_params=pltpu.CompilerParams(
            has_side_effects=True, vmem_limit_bytes=48 * 1024 * 1024
        ),
    )(table, src, rest, lift, inv)
    return (
        traces.reshape(source_trace.shape),
        coef.reshape(2, nsrc, LANES)[:, :, :nc],
    )


def solution(mesh):
    return jax.shard_map(
        functools.partial(per_device, mesh.shape["sy"], mesh.shape["sx"]),
        mesh=mesh,
        in_specs=(
            P(("wl", "sy"), "sx", None, None, None),
            P(("wl", "sy"), "sx", None, None, None, None),
            P(("wl", "sy"), "sx", None, None, None, None),
            P(("wl", "sy"), "sx", None, None, None, None),
            P("wl", None, None),
        ),
        out_specs=(P(("wl", "sy"), "sx", None, None, None, None), P("wl", None, None)),
        check_vma=False,
    )
```

```python
import functools

import jax
import jax.numpy as jnp
from jax import lax
from jax.experimental import pallas as pl
from jax.experimental.pallas import tpu as pltpu
from jax.sharding import PartitionSpec as P

ITERS = 6
LANES = 128
F32, BF16 = jnp.float32, jnp.bfloat16
MESH = pl.DeviceIdType.MESH
PRECISE = lax.Precision.HIGHEST
NT = (((1,), (1,)), ((), ()))


def dot(a, b):
    return jnp.dot(a, b, preferred_element_type=F32)


def dot_nt(a, b):
    return lax.dot_general(a, b, NT, preferred_element_type=F32)


def split(x):
    hi = x.astype(BF16)
    return hi, (x - hi.astype(F32)).astype(BF16)


def sweep_kernel(
    ny, nx, iters,
    map_ref, src_ref, rest_ref, lift_ref, inv_ref,
    traces_ref, coef_ref,
    out, recv, wrecv, cbuf, crecv, wcbuf, wcrecv, lhs, ext_lhs, ext_rhs,
    wts, part, xs, rowsum, ys,
    side_send, side_recv, diag_send, diag_recv,
    wside_send, wside_recv, wdiag_send, wdiag_recv,
    x_send, x_recv, y_send, y_recv, inv_full,
):
    rows, k = src_ref.shape
    side = k // 4
    nsrc = rows // 2
    nw_rows = rest_ref.shape[0]
    nc = nw_rows // 2
    half = nsrc // 2
    y, x = lax.axis_index("sy"), lax.axis_index("sx")
    up, dn, lf, rt = y > 0, y < ny - 1, x > 0, x < nx - 1
    sides = ((up, -1, 0), (dn, 1, 0), (lf, 0, -1), (rt, 0, 1))
    diags = (
        (up & lf, -1, -1),
        (up & rt, -1, 1),
        (dn & lf, 1, -1),
        (dn & rt, 1, 1),
    )

    def lanes(s):
        return pl.ds(s * side, side)

    def copies(src, dst, corner_src, corner_dst, ssem, rsem, dsem, drsem):
        flat, diag, flat_in, diag_in = [], [], [], []
        for d, (cond, dy, dx) in enumerate(sides):
            o = d ^ 1
            dev = {"sy": y + dy, "sx": x + dx}
            flat.append((cond, pltpu.make_async_remote_copy(
                src.at[:, lanes(d)], dst.at[:, lanes(o)], ssem.at[d], rsem.at[o],
                device_id=dev, device_id_type=MESH)))
            flat_in.append((cond, pltpu.make_async_remote_copy(
                src.at[:, lanes(d)], dst.at[:, lanes(d)], ssem.at[d], rsem.at[d],
                device_id=dev, device_id_type=MESH)))
        for d, (cond, dy, dx) in enumerate(diags):
            o = 3 - d
            dev = {"sy": y + dy, "sx": x + dx}
            diag.append((cond, pltpu.make_async_remote_copy(
                corner_src, corner_dst.at[o], dsem.at[d], drsem.at[o],
                device_id=dev, device_id_type=MESH)))
            diag_in.append((cond, pltpu.make_async_remote_copy(
                corner_src, corner_dst.at[d], dsem.at[d], drsem.at[d],
                device_id=dev, device_id_type=MESH)))
        return flat, diag, flat_in, diag_in

    def each(items, what):
        for cond, c in items:
            pl.when(cond)(getattr(c, what))

    def pack_corners(ref, dst, scale):
        def column(s, last):
            if last:
                return ref[:, (s + 1) * side - LANES:(s + 1) * side][:, LANES - 1:]
            return ref[:, s * side:s * side + LANES][:, 0:1]

        n = ref.shape[0]
        lane = lax.broadcasted_iota(jnp.int32, (n, LANES), 1)
        block = jnp.zeros((n, LANES), F32)
        for j, (a, b) in enumerate((
            ((0, 0), (2, 0)), ((0, 1), (3, 0)), ((1, 0), (2, 1)), ((1, 1), (3, 1)),
        )):
            block = jnp.where(lane == j, column(*a) + column(*b), block)
        if scale != 1.0:
            block = block * scale
        if n < LANES:
            block = jnp.concatenate([block, jnp.zeros((LANES - n, LANES), F32)], axis=0)
        dst[...] = block.T[:8]

    def assemble(get, get_corner, n, scale, write):
        row = lax.broadcasted_iota(jnp.int32, (LANES, LANES), 0)
        block = jnp.zeros((LANES, LANES), F32)
        for j in range(4):
            block = jnp.where(row == j, get_corner(j)[3 - j:4 - j], block)
        cols = block.T[:n] * scale
        lane = lax.broadcasted_iota(jnp.int32, (n, LANES), 1)
        ends = ((0, 1), (2, 3), (0, 2), (1, 3))
        for s in range(4):
            for t in range(side // LANES):
                at = s * side + t * LANES
                v = get(at)
                if t == 0:
                    j = ends[s][0]
                    v = v + jnp.where(lane == 0, cols[:, j:j + 1], 0.0)
                if t == side // LANES - 1:
                    j = ends[s][1]
                    v = v + jnp.where(lane == LANES - 1, cols[:, j:j + 1], 0.0)
                write(at, v)

    for d, (cond, _, _) in enumerate(sides):
        @pl.when(jnp.logical_not(cond))
        def _(d=d):
            for slot in range(2):
                recv[slot, :, lanes(d)] = jnp.zeros((rows, side), F32)
            wrecv[:, lanes(d)] = jnp.zeros((nw_rows, side), F32)
    for d, (cond, _, _) in enumerate(diags):
        @pl.when(jnp.logical_not(cond))
        def _(d=d):
            for slot in range(2):
                crecv[slot, d] = jnp.zeros((8, LANES), F32)
            wcrecv[d] = jnp.zeros((8, LANES), F32)

    w_flat, w_diag, w_flat_in, w_diag_in = copies(
        rest_ref, wrecv, wcbuf, wcrecv, wside_send, wside_recv, wdiag_send, wdiag_recv)
    pack_corners(rest_ref, wcbuf, 0.5)
    each(w_diag, "start")
    each(w_flat, "start")

    def exchange(slot, src):
        return copies(
            src, recv.at[slot], cbuf.at[slot], crecv.at[slot],
            side_send.at[slot], side_recv.at[slot], diag_send.at[slot], diag_recv.at[slot])

    def x_copies(slot):
        res = []
        for d in range(1, nx):
            peer = lax.rem(x + d, nx)
            res.append((
                pltpu.make_async_remote_copy(
                    part.at[slot], xs.at[slot, x], x_send.at[slot, d], x_recv.at[slot, d],
                    device_id={"sy": y, "sx": peer}, device_id_type=MESH),
                pltpu.make_async_remote_copy(
                    part.at[slot], xs.at[slot, lax.rem(x + nx - d, nx)],
                    x_send.at[slot, d], x_recv.at[slot, d],
                    device_id={"sy": y, "sx": peer}, device_id_type=MESH)))
        return res

    def y_copies(slot):
        res = []
        for d in range(1, ny):
            peer = lax.rem(y + d, ny)
            res.append((
                pltpu.make_async_remote_copy(
                    rowsum.at[slot], ys.at[slot, y], y_send.at[slot, d], y_recv.at[slot, d],
                    device_id={"sy": peer, "sx": x}, device_id_type=MESH),
                pltpu.make_async_remote_copy(
                    rowsum.at[slot], ys.at[slot, lax.rem(y + ny - d, ny)],
                    y_send.at[slot, d], y_recv.at[slot, d],
                    device_id={"sy": peer, "sx": x}, device_id_type=MESH)))
        return res

    def restrict_start(slot, src):
        re_hi, re_lo = split(src[:nsrc])
        im_hi, im_lo = split(src[nsrc:])
        a_hi, a_lo, b_hi, b_lo = (wts[i] for i in range(4))
        t = dot_nt(re_hi, a_hi) + dot_nt(im_hi, b_hi)
        t = t + (dot_nt(re_lo, a_hi) + dot_nt(im_lo, b_hi))
        t = t + (dot_nt(re_hi, a_lo) + dot_nt(im_hi, b_lo))
        lane = lax.broadcasted_iota(jnp.int32, (half, LANES), 1)
        t = jnp.where(lane < 2 * nc, t[:half], t[half:])
        part[slot] = t
        xs[slot, x] = t
        for c, _ in x_copies(slot):
            c.start()

    def restrict_turn(slot):
        for _, c in x_copies(slot):
            c.wait_recv()
        t = xs[slot, 0]
        for i in range(1, nx):
            t = t + xs[slot, i]
        rowsum[slot] = t
        ys[slot, y] = t
        for c, _ in y_copies(slot):
            c.start()

    def coarse(slot):
        for _, c in y_copies(slot):
            c.wait_recv()
        t = ys[slot, 0]
        for i in range(1, ny):
            t = t + ys[slot, i]
        lane = lax.broadcasted_iota(jnp.int32, (half, LANES), 1)
        low = lane < 2 * nc
        t = jnp.concatenate([jnp.where(low, t, 0.0), jnp.where(low, 0.0, t)], axis=0)
        c_re = jnp.dot(t, inv_full[0], preferred_element_type=F32, precision=PRECISE)
        c_im = jnp.dot(t, inv_full[1], preferred_element_type=F32, precision=PRECISE)
        c = jnp.concatenate([c_re, c_im], axis=0)
        coef_ref[0] = c_re[:, :nc]
        coef_ref[1] = c_im[:, :nc]
        hi, lo = split(c)
        lane = lax.broadcasted_iota(jnp.int32, (rows, LANES), 1)
        mid = (lane >= nc) & (lane < 2 * nc)
        ext_lhs[...] = jnp.where(mid, lo.astype(F32), hi.astype(F32)).astype(BF16)

    def restrict_end(slot):
        for c, _ in x_copies(slot):
            c.wait_send()
        for c, _ in y_copies(slot):
            c.wait_send()

    flat, diag, flat_in, diag_in = exchange(0, src_ref)
    pack_corners(src_ref, cbuf.at[0], 1.0)
    each(diag, "start")
    each(flat, "start")

    cr, ci = inv_ref[0], inv_ref[1]
    blank = jnp.zeros((nc, LANES - 3 * nc), F32)
    for i, (top, bottom) in enumerate(((cr, -ci), (ci, cr))):
        for j, v in enumerate((top, bottom, top, bottom)):
            inv_full[i, j * nc:(j + 1) * nc] = jnp.concatenate([v, v, v, blank], axis=1)

    lift_hi, lift_lo = split(lift_ref[...])
    lhs[...] = jnp.concatenate([lift_hi, lift_lo], axis=0)
    for s in range(4):
        p = dot(lhs[...], map_ref[:, s * side:(s + 1) * side])
        q = dot(lhs[...], map_ref[:, k + s * side:k + (s + 1) * side])
        p = p[:nw_rows] + p[nw_rows:]
        q = q[:nw_rows] + q[nw_rows:]
        for at, v in ((s * side, p[:nc] - q[nc:]), (k + s * side, q[:nc] + p[nc:])):
            hi, lo = split(v)
            ext_rhs[:, at:at + side] = jnp.concatenate(
                [hi, hi, lo, jnp.zeros((LANES - 3 * nc, side), BF16)], axis=0)

    each(w_flat_in, "wait_recv")
    each(w_diag_in, "wait_recv")

    def write_weights(at, v):
        wr, wi = v[:nc], v[nc:]
        for i, rowset in ((0, [wr, wi, wr, wi]), (2, [-wi, wr, -wi, wr])):
            hi, lo = split(jnp.concatenate(rowset, axis=0))
            wts[i, :, at:at + LANES] = hi
            wts[i + 1, :, at:at + LANES] = lo

    assemble(lambda at: wrecv[:, at:at + LANES], lambda j: wcrecv[j], nw_rows, 1.0, write_weights)
    restrict_start(0, src_ref)
    restrict_turn(0)
    each(w_flat, "wait_send")
    each(w_diag, "wait_send")

    def store_lhs(at, v):
        lhs[:, at:at + LANES] = v.astype(BF16)

    def step(it, carry):
        old = lax.rem(it + 1, 2)
        new = lax.rem(it, 2)
        flat, diag, flat_in, diag_in = exchange(old, out)
        each(diag_in, "wait_recv")
        each(flat_in, "wait_recv")
        assemble(lambda at: recv[old, :, at:at + LANES], lambda j: crecv[old, j], rows, 0.5, store_lhs)
        each(flat, "wait_send")
        each(diag, "wait_send")
        for s in range(4):
            at = s * side
            p = dot(lhs[...], map_ref[:, at:at + side])
            q = dot(lhs[...], map_ref[:, k + at:k + at + side])
            out[:nsrc, at:at + side] = p[:nsrc] - q[nsrc:] + src_ref[:nsrc, at:at + side]
            out[nsrc:, at:at + side] = q[:nsrc] + p[nsrc:] + src_ref[nsrc:, at:at + side]
        coarse(old)
        restrict_end(old)
        for s in range(4):
            at = s * side
            p = dot(ext_lhs[...], ext_rhs[:, at:at + side])
            q = dot(ext_lhs[...], ext_rhs[:, k + at:k + at + side])
            out[:nsrc, at:at + side] += p[:nsrc] - q[nsrc:]
            out[nsrc:, at:at + side] += q[:nsrc] + p[nsrc:]
        flat, diag, _, _ = exchange(new, out)
        pack_corners(out, cbuf.at[new], 1.0)
        each(diag, "start")

        @pl.when(it < iters - 1)
        def _():
            restrict_start(new, out)

        each(flat, "start")

        @pl.when(it < iters - 1)
        def _():
            restrict_turn(new)

        return carry

    lax.fori_loop(1, iters, step, 0)

    last = (iters - 1) % 2
    flat, diag, flat_in, diag_in = exchange(last, out)
    each(diag_in, "wait_recv")
    each(flat_in, "wait_recv")

    def store_out(at, v):
        traces_ref[:, at:at + LANES] = v

    assemble(lambda at: recv[last, :, at:at + LANES], lambda j: crecv[last, j], rows, 0.5, store_out)
    each(flat, "wait_send")
    each(diag, "wait_send")


def per_device(ny, nx, interface_map, source_trace, restriction, prolongation, coarse_inverse):
    _, _, _, nsrc, _, side = source_trace.shape
    nc = restriction.shape[3]
    k, rows = 4 * side, 2 * nsrc
    table = interface_map.reshape(k, 2 * k)
    src = source_trace.reshape(rows, k)
    rest = restriction.reshape(2 * nc, k)
    lift = prolongation.reshape(2 * nc, k)
    half = nsrc // 2
    dma = pltpu.SemaphoreType.DMA
    vmem = pl.BlockSpec(memory_space=pltpu.VMEM)
    traces, coef = pl.pallas_call(
        functools.partial(sweep_kernel, ny, nx, ITERS),
        out_shape=(
            jax.ShapeDtypeStruct((rows, k), F32),
            jax.ShapeDtypeStruct((2, nsrc, nc), F32),
        ),
        in_specs=[vmem] * 5,
        out_specs=(vmem, vmem),
        scratch_shapes=[
            pltpu.VMEM((rows, k), F32),
            pltpu.VMEM((2, rows, k), F32),
            pltpu.VMEM((2 * nc, k), F32),
            pltpu.VMEM((2, 8, LANES), F32),
            pltpu.VMEM((2, 4, 8, LANES), F32),
            pltpu.VMEM((8, LANES), F32),
            pltpu.VMEM((4, 8, LANES), F32),
            pltpu.VMEM((rows, k), BF16),
            pltpu.VMEM((rows, LANES), BF16),
            pltpu.VMEM((LANES, 2 * k), BF16),
            pltpu.VMEM((4, 4 * nc, k), BF16),
            pltpu.VMEM((2, half, LANES), F32),
            pltpu.VMEM((2, nx, half, LANES), F32),
            pltpu.VMEM((2, half, LANES), F32),
            pltpu.VMEM((2, ny, half, LANES), F32),
            dma((2, 4)), dma((2, 4)), dma((2, 4)), dma((2, 4)),
            dma((4,)), dma((4,)), dma((4,)), dma((4,)),
            dma((2, nx)), dma((2, nx)), dma((2, ny)), dma((2, ny)),
            pltpu.VMEM((2, 4 * nc, LANES), F32),
        ],
        compiler_params=pltpu.CompilerParams(
            has_side_effects=True, vmem_limit_bytes=48 * 1024 * 1024
        ),
    )(table, src, rest, lift, coarse_inverse)
    return (
        traces.reshape(source_trace.shape),
        coef,
    )


def solution(mesh):
    return jax.shard_map(
        functools.partial(per_device, mesh.shape["sy"], mesh.shape["sx"]),
        mesh=mesh,
        in_specs=(
            P(("wl", "sy"), "sx", None, None, None),
            P(("wl", "sy"), "sx", None, None, None, None),
            P(("wl", "sy"), "sx", None, None, None, None),
            P(("wl", "sy"), "sx", None, None, None, None),
            P("wl", None, None),
        ),
        out_specs=(P(("wl", "sy"), "sx", None, None, None, None), P("wl", None, None)),
        check_vma=False,
    )
```

```python
import functools

import jax
import jax.numpy as jnp
from jax import lax
from jax.experimental import pallas as pl
from jax.experimental.pallas import tpu as pltpu
from jax.sharding import PartitionSpec as P

ITERS = 6
LANES = 128
F32, BF16 = jnp.float32, jnp.bfloat16
MESH = pl.DeviceIdType.MESH
PRECISE = lax.Precision.HIGHEST
NT = (((1,), (1,)), ((), ()))


def dot(a, b):
    return jnp.dot(a, b, preferred_element_type=F32)


def dot_nt(a, b):
    return lax.dot_general(a, b, NT, preferred_element_type=F32)


def split(x):
    hi = x.astype(BF16)
    return hi, (x - hi.astype(F32)).astype(BF16)


def sweep_kernel(
    ny, nx, iters,
    map_ref, src_ref, rest_ref, lift_ref, inv_ref,
    traces_ref, coef_ref,
    out, recv, wrecv, cbuf, crecv, wcbuf, wcrecv, lhs, ext_lhs, ext_rhs,
    wts, part, xs, rowsum, ys,
    side_send, side_recv, diag_send, diag_recv,
    wside_send, wside_recv, wdiag_send, wdiag_recv,
    x_send, x_recv, y_send, y_recv, inv_full,
):
    rows, k = src_ref.shape
    side = k // 4
    nsrc = rows // 2
    nw_rows = rest_ref.shape[0]
    nc = nw_rows // 2
    half = nsrc // 2
    y, x = lax.axis_index("sy"), lax.axis_index("sx")
    up, dn, lf, rt = y > 0, y < ny - 1, x > 0, x < nx - 1
    sides = ((up, -1, 0), (dn, 1, 0), (lf, 0, -1), (rt, 0, 1))
    diags = (
        (up & lf, -1, -1),
        (up & rt, -1, 1),
        (dn & lf, 1, -1),
        (dn & rt, 1, 1),
    )

    def lanes(s):
        return pl.ds(s * side, side)

    def copies(src, dst, corner_src, corner_dst, ssem, rsem, dsem, drsem):
        flat, diag, flat_in, diag_in = [], [], [], []
        for d, (cond, dy, dx) in enumerate(sides):
            o = d ^ 1
            dev = {"sy": y + dy, "sx": x + dx}
            flat.append((cond, pltpu.make_async_remote_copy(
                src.at[:, lanes(d)], dst.at[:, lanes(o)], ssem.at[d], rsem.at[o],
                device_id=dev, device_id_type=MESH)))
            flat_in.append((cond, pltpu.make_async_remote_copy(
                src.at[:, lanes(d)], dst.at[:, lanes(d)], ssem.at[d], rsem.at[d],
                device_id=dev, device_id_type=MESH)))
        for d, (cond, dy, dx) in enumerate(diags):
            o = 3 - d
            dev = {"sy": y + dy, "sx": x + dx}
            diag.append((cond, pltpu.make_async_remote_copy(
                corner_src, corner_dst.at[o], dsem.at[d], drsem.at[o],
                device_id=dev, device_id_type=MESH)))
            diag_in.append((cond, pltpu.make_async_remote_copy(
                corner_src, corner_dst.at[d], dsem.at[d], drsem.at[d],
                device_id=dev, device_id_type=MESH)))
        return flat, diag, flat_in, diag_in

    def each(items, what):
        for cond, c in items:
            pl.when(cond)(getattr(c, what))

    def pack_corners(ref, dst, scale):
        def column(s, last):
            if last:
                return ref[:, (s + 1) * side - LANES:(s + 1) * side][:, LANES - 1:]
            return ref[:, s * side:s * side + LANES][:, 0:1]

        n = ref.shape[0]
        lane = lax.broadcasted_iota(jnp.int32, (n, LANES), 1)
        block = jnp.zeros((n, LANES), F32)
        for j, (a, b) in enumerate((
            ((0, 0), (2, 0)), ((0, 1), (3, 0)), ((1, 0), (2, 1)), ((1, 1), (3, 1)),
        )):
            block = jnp.where(lane == j, column(*a) + column(*b), block)
        if scale != 1.0:
            block = block * scale
        if n < LANES:
            block = jnp.concatenate([block, jnp.zeros((LANES - n, LANES), F32)], axis=0)
        dst[...] = block.T[:8]

    def assemble(get, get_corner, n, scale, write):
        row = lax.broadcasted_iota(jnp.int32, (LANES, LANES), 0)
        block = jnp.zeros((LANES, LANES), F32)
        for j in range(4):
            block = jnp.where(row == j, get_corner(j)[3 - j:4 - j], block)
        cols = block.T[:n] * scale
        lane = lax.broadcasted_iota(jnp.int32, (n, LANES), 1)
        ends = ((0, 1), (2, 3), (0, 2), (1, 3))
        for s in range(4):
            for t in range(side // LANES):
                at = s * side + t * LANES
                v = get(at)
                if t == 0:
                    j = ends[s][0]
                    v = v + jnp.where(lane == 0, cols[:, j:j + 1], 0.0)
                if t == side // LANES - 1:
                    j = ends[s][1]
                    v = v + jnp.where(lane == LANES - 1, cols[:, j:j + 1], 0.0)
                write(at, v)

    for d, (cond, _, _) in enumerate(sides):
        @pl.when(jnp.logical_not(cond))
        def _(d=d):
            for slot in range(2):
                recv[slot, :, lanes(d)] = jnp.zeros((rows, side), F32)
            wrecv[:, lanes(d)] = jnp.zeros((nw_rows, side), F32)
    for d, (cond, _, _) in enumerate(diags):
        @pl.when(jnp.logical_not(cond))
        def _(d=d):
            for slot in range(2):
                crecv[slot, d] = jnp.zeros((8, LANES), F32)
            wcrecv[d] = jnp.zeros((8, LANES), F32)

    w_flat, w_diag, w_flat_in, w_diag_in = copies(
        rest_ref, wrecv, wcbuf, wcrecv, wside_send, wside_recv, wdiag_send, wdiag_recv)
    pack_corners(rest_ref, wcbuf, 0.5)
    each(w_diag, "start")
    each(w_flat, "start")

    def exchange(slot, src):
        return copies(
            src, recv.at[slot], cbuf.at[slot], crecv.at[slot],
            side_send.at[slot], side_recv.at[slot], diag_send.at[slot], diag_recv.at[slot])

    def x_copies(slot):
        res = []
        for d in range(1, nx):
            peer = lax.rem(x + d, nx)
            res.append((
                pltpu.make_async_remote_copy(
                    part.at[slot], xs.at[slot, x], x_send.at[slot, d], x_recv.at[slot, d],
                    device_id={"sy": y, "sx": peer}, device_id_type=MESH),
                pltpu.make_async_remote_copy(
                    part.at[slot], xs.at[slot, lax.rem(x + nx - d, nx)],
                    x_send.at[slot, d], x_recv.at[slot, d],
                    device_id={"sy": y, "sx": peer}, device_id_type=MESH)))
        return res

    def y_copies(slot):
        res = []
        for d in range(1, ny):
            peer = lax.rem(y + d, ny)
            res.append((
                pltpu.make_async_remote_copy(
                    rowsum.at[slot], ys.at[slot, y], y_send.at[slot, d], y_recv.at[slot, d],
                    device_id={"sy": peer, "sx": x}, device_id_type=MESH),
                pltpu.make_async_remote_copy(
                    rowsum.at[slot], ys.at[slot, lax.rem(y + ny - d, ny)],
                    y_send.at[slot, d], y_recv.at[slot, d],
                    device_id={"sy": peer, "sx": x}, device_id_type=MESH)))
        return res

    def restrict_start(slot, src):
        re_hi, re_lo = split(src[:nsrc])
        im_hi, im_lo = split(src[nsrc:])
        a_hi, a_lo, b_hi, b_lo = (wts[i] for i in range(4))
        t = dot_nt(re_hi, a_hi) + dot_nt(im_hi, b_hi)
        t = t + (dot_nt(re_lo, a_hi) + dot_nt(im_lo, b_hi))
        t = t + (dot_nt(re_hi, a_lo) + dot_nt(im_hi, b_lo))
        lane = lax.broadcasted_iota(jnp.int32, (half, LANES), 1)
        t = jnp.where(lane < 2 * nc, t[:half], t[half:])
        part[slot] = t
        xs[slot, x] = t
        for c, _ in x_copies(slot):
            c.start()

    def restrict_turn(slot):
        for _, c in x_copies(slot):
            c.wait_recv()
        t = xs[slot, 0]
        for i in range(1, nx):
            t = t + xs[slot, i]
        rowsum[slot] = t
        ys[slot, y] = t
        for c, _ in y_copies(slot):
            c.start()

    def coarse(slot):
        for _, c in y_copies(slot):
            c.wait_recv()
        t = ys[slot, 0]
        for i in range(1, ny):
            t = t + ys[slot, i]
        lane = lax.broadcasted_iota(jnp.int32, (half, LANES), 1)
        low = lane < 2 * nc
        t = jnp.concatenate([jnp.where(low, t, 0.0), jnp.where(low, 0.0, t)], axis=0)
        c_re = jnp.dot(t, inv_full[0], preferred_element_type=F32, precision=PRECISE)
        c_im = jnp.dot(t, inv_full[1], preferred_element_type=F32, precision=PRECISE)
        c = jnp.concatenate([c_re, c_im], axis=0)
        coef_ref[0] = c_re[:, :nc]
        coef_ref[1] = c_im[:, :nc]
        hi, lo = split(c)
        lane = lax.broadcasted_iota(jnp.int32, (rows, LANES), 1)
        mid = (lane >= nc) & (lane < 2 * nc)
        ext_lhs[...] = jnp.where(mid, lo.astype(F32), hi.astype(F32)).astype(BF16)

    def restrict_end(slot):
        for c, _ in x_copies(slot):
            c.wait_send()
        for c, _ in y_copies(slot):
            c.wait_send()

    flat, diag, flat_in, diag_in = exchange(0, src_ref)
    pack_corners(src_ref, cbuf.at[0], 1.0)
    each(diag, "start")
    each(flat, "start")

    cr, ci = inv_ref[0], inv_ref[1]
    blank = jnp.zeros((nc, LANES - 3 * nc), F32)
    for i, (top, bottom) in enumerate(((cr, -ci), (ci, cr))):
        for j, v in enumerate((top, bottom, top, bottom)):
            inv_full[i, j * nc:(j + 1) * nc] = jnp.concatenate([v, v, v, blank], axis=1)

    lift_hi, lift_lo = split(lift_ref[...])
    lhs[...] = jnp.concatenate([lift_hi, lift_lo], axis=0)
    for s in range(4):
        p = dot(lhs[...], map_ref[:, s * side:(s + 1) * side])
        q = dot(lhs[...], map_ref[:, k + s * side:k + (s + 1) * side])
        p = p[:nw_rows] + p[nw_rows:]
        q = q[:nw_rows] + q[nw_rows:]
        for at, v in ((s * side, p[:nc] - q[nc:]), (k + s * side, q[:nc] + p[nc:])):
            hi, lo = split(v)
            ext_rhs[:, at:at + side] = jnp.concatenate(
                [hi, hi, lo, jnp.zeros((LANES - 3 * nc, side), BF16)], axis=0)

    each(w_flat_in, "wait_recv")
    each(w_diag_in, "wait_recv")

    def write_weights(at, v):
        wr, wi = v[:nc], v[nc:]
        for i, rowset in ((0, [wr, wi, wr, wi]), (2, [-wi, wr, -wi, wr])):
            hi, lo = split(jnp.concatenate(rowset, axis=0))
            wts[i, :, at:at + LANES] = hi
            wts[i + 1, :, at:at + LANES] = lo

    assemble(lambda at: wrecv[:, at:at + LANES], lambda j: wcrecv[j], nw_rows, 1.0, write_weights)
    restrict_start(0, src_ref)
    restrict_turn(0)
    each(w_flat, "wait_send")
    each(w_diag, "wait_send")

    def store_lhs(at, v):
        lhs[:, at:at + LANES] = v.astype(BF16)

    def step(it, carry):
        old = lax.rem(it + 1, 2)
        new = lax.rem(it, 2)
        flat, diag, flat_in, diag_in = exchange(old, out)
        each(diag_in, "wait_recv")
        each(flat_in, "wait_recv")
        assemble(lambda at: recv[old, :, at:at + LANES], lambda j: crecv[old, j], rows, 0.5, store_lhs)
        each(flat, "wait_send")
        each(diag, "wait_send")
        for s in range(4):
            at = s * side
            p = dot(lhs[...], map_ref[:, at:at + side])
            q = dot(lhs[...], map_ref[:, k + at:k + at + side])
            out[:nsrc, at:at + side] = p[:nsrc] - q[nsrc:] + src_ref[:nsrc, at:at + side]
            out[nsrc:, at:at + side] = q[:nsrc] + p[nsrc:] + src_ref[nsrc:, at:at + side]
        coarse(old)
        restrict_end(old)
        for s in range(4):
            at = s * side
            p = dot(ext_lhs[...], ext_rhs[:, at:at + side])
            q = dot(ext_lhs[...], ext_rhs[:, k + at:k + at + side])
            out[:nsrc, at:at + side] += p[:nsrc] - q[nsrc:]
            out[nsrc:, at:at + side] += q[:nsrc] + p[nsrc:]
        flat, diag, _, _ = exchange(new, out)
        pack_corners(out, cbuf.at[new], 1.0)
        each(diag, "start")

        each(flat, "start")

        @pl.when(it < iters - 1)
        def _():
            restrict_start(new, out)
            restrict_turn(new)

        return carry

    lax.fori_loop(1, iters, step, 0)

    last = (iters - 1) % 2
    flat, diag, flat_in, diag_in = exchange(last, out)
    each(diag_in, "wait_recv")
    each(flat_in, "wait_recv")

    def store_out(at, v):
        traces_ref[:, at:at + LANES] = v

    assemble(lambda at: recv[last, :, at:at + LANES], lambda j: crecv[last, j], rows, 0.5, store_out)
    each(flat, "wait_send")
    each(diag, "wait_send")


def per_device(ny, nx, interface_map, source_trace, restriction, prolongation, coarse_inverse):
    _, _, _, nsrc, _, side = source_trace.shape
    nc = restriction.shape[3]
    k, rows = 4 * side, 2 * nsrc
    table = interface_map.reshape(k, 2 * k)
    src = source_trace.reshape(rows, k)
    rest = restriction.reshape(2 * nc, k)
    lift = prolongation.reshape(2 * nc, k)
    half = nsrc // 2
    dma = pltpu.SemaphoreType.DMA
    vmem = pl.BlockSpec(memory_space=pltpu.VMEM)
    traces, coef = pl.pallas_call(
        functools.partial(sweep_kernel, ny, nx, ITERS),
        out_shape=(
            jax.ShapeDtypeStruct((rows, k), F32),
            jax.ShapeDtypeStruct((2, nsrc, nc), F32),
        ),
        in_specs=[vmem] * 5,
        out_specs=(vmem, vmem),
        scratch_shapes=[
            pltpu.VMEM((rows, k), F32),
            pltpu.VMEM((2, rows, k), F32),
            pltpu.VMEM((2 * nc, k), F32),
            pltpu.VMEM((2, 8, LANES), F32),
            pltpu.VMEM((2, 4, 8, LANES), F32),
            pltpu.VMEM((8, LANES), F32),
            pltpu.VMEM((4, 8, LANES), F32),
            pltpu.VMEM((rows, k), BF16),
            pltpu.VMEM((rows, LANES), BF16),
            pltpu.VMEM((LANES, 2 * k), BF16),
            pltpu.VMEM((4, 4 * nc, k), BF16),
            pltpu.VMEM((2, half, LANES), F32),
            pltpu.VMEM((2, nx, half, LANES), F32),
            pltpu.VMEM((2, half, LANES), F32),
            pltpu.VMEM((2, ny, half, LANES), F32),
            dma((2, 4)), dma((2, 4)), dma((2, 4)), dma((2, 4)),
            dma((4,)), dma((4,)), dma((4,)), dma((4,)),
            dma((2, nx)), dma((2, nx)), dma((2, ny)), dma((2, ny)),
            pltpu.VMEM((2, 4 * nc, LANES), F32),
        ],
        compiler_params=pltpu.CompilerParams(
            has_side_effects=True, vmem_limit_bytes=48 * 1024 * 1024
        ),
    )(table, src, rest, lift, coarse_inverse)
    return (
        traces.reshape(source_trace.shape),
        coef,
    )


def solution(mesh):
    return jax.shard_map(
        functools.partial(per_device, mesh.shape["sy"], mesh.shape["sx"]),
        mesh=mesh,
        in_specs=(
            P(("wl", "sy"), "sx", None, None, None),
            P(("wl", "sy"), "sx", None, None, None, None),
            P(("wl", "sy"), "sx", None, None, None, None),
            P(("wl", "sy"), "sx", None, None, None, None),
            P("wl", None, None),
        ),
        out_specs=(P(("wl", "sy"), "sx", None, None, None, None), P("wl", None, None)),
        check_vma=False,
    )
```
